32 devices in a mesh: gy: 8 (over z, y), gz: 4 (over x, core).
Axes of the slice: x: 2, y: 2, z: 4, core: 2. Of those that a mesh axis runs over, the one named last changes fastest.
Arguments:
- tokens: bfloat16 [2, 64, 8, 8, 1024], P(None, None, 'gy', 'gz'), may hold values from -64 to 64
- w_qkv: bfloat16 [1024, 3072], P('gy'), may hold values from -2 to 2
- w_out: bfloat16 [1024, 1024], P('gy'), may hold values from -0.1875 to 0.1875
- bias_x: float32 [16, 127], replicated, may hold values from -4 to 4
- bias_y: float32 [16, 15], replicated, may hold values from -4 to 4
- bias_z: float32 [16, 15], replicated, may hold values from -4 to 4
Outputs:
- mixed: bfloat16 [2, 64, 8, 8, 1024], P(None, None, 'gy', 'gz')
The draws below stay inside these ranges and needn't reach their ends.
All inputs are finite; a program needn't handle non-finite values.
Results may differ from the reference program's by a relative error of at most 0.0083.
Values may be sent and summed in bfloat16 or wider, within the bound.
A program may use at most 64 MiB of HBM per device.

```python
import math
import jax
import jax.numpy as jnp
from jax import lax

D = 1024
HEADS = 16
HEAD = 64
SAMPLES = 2
NX = 64
NY = 8
NZ = 8


def draw_tokens(key, part):
    streams = jax.random.split(jax.random.fold_in(key, 11), 1)
    dims = (SAMPLES, NX, NY, NZ, D)
    values = jax.random.normal(streams[0], dims, jnp.float32)
    values = values * 0.25
    return jnp.clip(values, -64.0, 64.0).astype(jnp.bfloat16)


def draw_w_qkv(key, part):
    limit = 6.0 / math.sqrt(D)
    base = jax.random.normal(jax.random.fold_in(key, 12), (D, 3 * D), jnp.float32) / math.sqrt(D)
    base = jnp.clip(base, -limit, limit)
    return jnp.clip(base, -2.0, 2.0).astype(jnp.bfloat16)


def levels(stream_key, extent, cuts, smallest, top_value):
    gain, own = 1.0, jax.random.fold_in(stream_key, 6)
    for position, blocks in cuts:
        steps = jnp.exp(jax.random.uniform(jax.random.fold_in(own, position), (blocks,), jnp.float32, smallest / len(cuts), top_value / len(cuts)))
        gain = gain * jnp.repeat(steps, extent[position] // blocks).reshape([-1 if axis == position else 1 for axis in range(len(extent))])
    return gain


def normal_values(own_key, extent, scale, most, cuts=(), held_as=jnp.bfloat16):
    values = jax.random.normal(own_key, extent, jnp.float32) * scale
    if len(cuts) > 0:
        values = levels(own_key, extent, cuts, -0.22, 0.18) * values
    return jnp.clip(values, min=-most, max=most).astype(held_as)


def setup_inputs(seed: int = 0) -> dict:
    splits = jax.random.split(jax.random.key(seed), 7)
    return {
        "tokens": draw_tokens(jax.random.fold_in(splits[6], 71), 0),
        "w_qkv": draw_w_qkv(jax.random.fold_in(splits[6], 71), 0),
        "w_out": normal_values(splits[2], (D, D), D ** -0.5, 0.1875, ((0, 8),)),
        "bias_x": normal_values(splits[3], (HEADS, 2 * NX - 1), 1.0, 4.0, (), jnp.float32),
        "bias_y": normal_values(splits[4], (HEADS, 2 * NY - 1), 1.0, 4.0, (), jnp.float32),
        "bias_z": normal_values(splits[5], (HEADS, 2 * NZ - 1), 1.0, 4.0, (), jnp.float32),
    }


einsum_forms = {1: ('bxyzhs,bwyzhs->byzhxw', 'byzhxw,bwyzhs->bxyzhs'), 2: ('bxyzhs,bxwzhs->bxzhyw', 'bxzhyw,bxwzhs->bxyzhs'), 3: ('bxyzhs,bxywhs->bxyhzw', 'bxyhzw,bxywhs->bxyzhs')}

def norm_rows(tokens):
    values = tokens.astype(jnp.float32)
    center = lax.optimization_barrier(jnp.mean(values, axis=-1, keepdims=True))
    spread = lax.optimization_barrier(jnp.mean((values - center) ** 2, axis=-1, keepdims=True))
    return ((values - center) * lax.rsqrt(spread + 1e-05)).astype(jnp.bfloat16)

def rel_bias(table):
    length = (table.shape[1] + 1) // 2
    offsets = jnp.arange(length)[:, None] - jnp.arange(length)[None, :] + length - 1
    return table[:, offsets.astype(jnp.int32)]

def attend(qkv, table, axis):
    dims = qkv.shape
    features = dims[-1] // 3
    parts = qkv.reshape(dims[:-1] + (3, HEADS, HEAD))
    query = parts[..., 0, :, :].astype(jnp.float32)
    keys = parts[..., 1, :, :].astype(jnp.float32)
    values = parts[..., 2, :, :].astype(jnp.float32)
    score_form, mix_form = einsum_forms[axis]
    scores = jnp.einsum(score_form, query, keys) * HEAD ** (-0.5) + rel_bias(table)
    scores = scores - lax.optimization_barrier(jnp.max(scores, axis=-1, keepdims=True))
    expo = jnp.exp(scores)
    weights = (expo / lax.optimization_barrier(jnp.sum(expo, axis=-1, keepdims=True))).astype(jnp.bfloat16)
    mixed = jnp.einsum(mix_form, weights.astype(jnp.float32), values)
    return mixed.reshape(dims[:-1] + (features,)).astype(jnp.bfloat16)

def reference(tokens, w_qkv, w_out, bias_x, bias_y, bias_z):

    def one_sample(sample):
        normed = norm_rows(sample)
        qkv = jnp.dot(normed.reshape(-1, D), w_qkv, preferred_element_type=jnp.float32)
        qkv = qkv.astype(jnp.bfloat16).reshape((1, NX, NY, NZ, 3 * D))
        along_x = attend(qkv, bias_x, 1).astype(jnp.float32)
        along_y = attend(qkv, bias_y, 2).astype(jnp.float32)
        along_z = attend(qkv, bias_z, 3).astype(jnp.float32)
        summed = (along_x + along_y + along_z).astype(jnp.bfloat16).reshape(-1, D)
        result = jnp.dot(summed, w_out, preferred_element_type=jnp.float32)
        result = result + sample.reshape(-1, D).astype(jnp.float32)
        return result.astype(jnp.bfloat16).reshape((NX, NY, NZ, D))
    return lax.map(one_sample, tokens)
```

```python
import functools

import jax
import jax.numpy as jnp
import numpy as np
from jax import lax
from jax.experimental import pallas as pl
from jax.experimental.pallas import tpu as pltpu
from jax.sharding import PartitionSpec as P

HEADS = 16
HEAD = 64


einsum_forms = {
    1: ("bxyzhs,bwyzhs->byzhxw", "byzhxw,bwyzhs->bxyzhs"),
    2: ("bxyzhs,bxwzhs->bxzhyw", "bxzhyw,bxwzhs->bxyzhs"),
    3: ("bxyzhs,bxywhs->bxyhzw", "bxyhzw,bxywhs->bxyzhs"),
}


def norm_rows(tokens):
    values = tokens.astype(jnp.float32)
    center = jnp.mean(values, axis=-1, keepdims=True)
    spread = jnp.mean((values - center) ** 2, axis=-1, keepdims=True)
    return ((values - center) * lax.rsqrt(spread + 1e-05)).astype(jnp.bfloat16)


def rel_bias(table):
    length = (table.shape[1] + 1) // 2
    offsets = (
        lax.broadcasted_iota(jnp.int32, (length, length), 0)
        - lax.broadcasted_iota(jnp.int32, (length, length), 1)
        + length
        - 1
    )
    lookup = (
        offsets[:, :, None] == lax.broadcasted_iota(jnp.int32, (1, 1, 2 * length - 1), 2)
    ).astype(jnp.float32)
    return jnp.einsum("hr,ijr->hij", table, lookup, precision=lax.Precision.HIGHEST)


def attend(qkv, table, axis):
    dims = qkv.shape
    features = dims[-1] // 3
    parts = qkv.reshape(dims[:-1] + (3, HEADS, HEAD))
    query = parts[..., 0, :, :]
    keys = parts[..., 1, :, :]
    values = parts[..., 2, :, :]
    score_form, mix_form = einsum_forms[axis]
    scores = jnp.einsum(score_form, query, keys, preferred_element_type=jnp.float32) * HEAD ** (
        -0.5
    ) + rel_bias(table)
    scores = scores - jnp.max(scores, axis=-1, keepdims=True)
    expo = jnp.exp(scores)
    weights = (expo / jnp.sum(expo, axis=-1, keepdims=True)).astype(jnp.bfloat16)
    mixed = jnp.einsum(mix_form, weights, values, preferred_element_type=jnp.float32)
    return mixed.reshape(dims[:-1] + (features,)).astype(jnp.bfloat16)


def return_y(result):
    return lax.all_to_all(result, "gy", split_axis=2, concat_axis=1, tiled=True)


def return_z(result):
    return lax.all_to_all(result, "gz", split_axis=3, concat_axis=1, tiled=True)


def shards(tokens, w_qkv, w_out, bias_x, bias_y, bias_z):
    samples, depth, rows_y, rows_z, features = tokens.shape
    normed = norm_rows(tokens)
    gathered = lax.all_gather(w_qkv, "gy", axis=0, tiled=True)

    def project(inputs):
        product = jnp.dot(
            inputs.reshape(-1, features), gathered, preferred_element_type=jnp.float32
        )
        return product.astype(jnp.bfloat16).reshape(inputs.shape[:-1] + (3 * features,))

    along_x = attend(project(normed), bias_x, 1)
    along_y = return_y(
        attend(
            project(lax.all_to_all(normed, "gy", split_axis=1, concat_axis=2, tiled=True)),
            bias_y,
            2,
        )
    )
    along_z = return_z(
        attend(
            project(lax.all_to_all(normed, "gz", split_axis=1, concat_axis=3, tiled=True)),
            bias_z,
            3,
        )
    )
    summed = along_x.astype(jnp.float32) + along_y.astype(jnp.float32) + along_z.astype(jnp.float32)
    summed = summed.astype(jnp.bfloat16).reshape(-1, features)
    residual = tokens.reshape(-1, features).astype(jnp.float32)
    result = residual + jnp.dot(
        summed, lax.all_gather(w_out, "gy", axis=0, tiled=True), preferred_element_type=jnp.float32
    )
    return result.astype(jnp.bfloat16).reshape(tokens.shape)


def device(**where):
    return {"device_id": where, "device_id_type": pl.DeviceIdType.MESH}


def greet(me_y, me_z, size_y, size_z):
    barrier = pltpu.get_barrier_semaphore()
    for step in range(1, size_y):
        pl.semaphore_signal(barrier, inc=1, **device(gy=lax.rem(me_y + step, size_y)))
    for step in range(1, size_z):
        pl.semaphore_signal(barrier, inc=1, **device(gz=lax.rem(me_z + step, size_z)))
    pl.semaphore_wait(barrier, size_y + size_z - 2)


def exchange(source, target, axis, me, size, send_sems, recv_sems):
    rows = source.shape[1] // size
    copies = []
    for step in range(1, size):
        peer = lax.rem(me + step, size)
        copies.append(
            pltpu.make_async_remote_copy(
                src_ref=source.at[:, pl.ds(pl.multiple_of(peer * rows, rows), rows), :],
                dst_ref=target.at[:, pl.ds(pl.multiple_of(me * rows, rows), rows), :],
                send_sem=send_sems.at[step - 1],
                recv_sem=recv_sems.at[step - 1],
                **device(**{axis: peer}),
            )
        )
    for copy in copies:
        copy.start()
    return copies


def keep_own(source, target, me, size):
    rows = source.shape[1] // size
    own = pl.ds(pl.multiple_of(me * rows, rows), rows)
    target[:, own, :] = source[:, own, :]


def gather_kernel(
    size_y, size_z, tokens, w_qkv, w_out, along, all_qkv, all_out,
    y_send, y_recv, z_send, z_recv, up_send, up_recv, down_send, down_recv,
    side_send, side_recv, core_send, core_recv, own_sem,
):
    me_y, me_z = lax.axis_index("gy"), lax.axis_index("gz")
    depth = w_qkv.shape[0]
    half = depth // 2
    levels = size_y // 2
    level, side, core = me_y // 2, lax.rem(me_y, 2), lax.rem(me_z, 2)
    values = tokens[...].astype(jnp.float32)
    center = jnp.mean(values, axis=-1, keepdims=True)
    spread = jnp.mean((values - center) ** 2, axis=-1, keepdims=True)
    along[0] = ((values - center) * lax.rsqrt(spread + 1e-05)).astype(jnp.bfloat16)
    pairs = ((w_qkv, all_qkv), (w_out, all_out))

    greet(me_y, me_z, size_y, size_z)

    def rows_of(lev, sid):
        return pl.ds(pl.multiple_of((lev * 2 + sid) * depth + core * half, half), half)

    def transfer(array, lev, sid, sends, recvs, slot, where, own=False):
        block = pairs[array][1].at[rows_of(lev, sid), :]
        source = pairs[array][0].at[pl.ds(pl.multiple_of(core * half, half), half), :] if own else block
        return pltpu.make_async_remote_copy(
            src_ref=source, dst_ref=block, send_sem=sends.at[array, slot],
            recv_sem=recvs.at[array, slot], **device(**where),
        )

    above = {"gy": me_y + 2}
    below = {"gy": me_y - 2}
    beside = {"gy": level * 2 + 1 - side}
    twin = {"gz": me_z + 1 - 2 * core}

    def up(array, step, own=False):
        return transfer(array, level - step, side, up_send, up_recv, step, above, own)

    def down(array, step, own=False):
        return transfer(array, level + step, side, down_send, down_recv, step, below, own)

    def across(array, lev, own=False):
        return transfer(array, lev, side, side_send, side_recv, lev, beside, own)

    def share(array, lev, sid, own=False):
        return transfer(array, lev, sid, core_send, core_recv, lev * 2 + sid, twin, own)

    sent_y = exchange(along.at[0], along.at[1], "gy", me_y, size_y, y_send, y_recv)
    sent_z = exchange(along.at[0], along.at[2], "gz", me_z, size_z, z_send, z_recv)
    for array in (0, 1):
        pl.when(level + 1 < levels)(lambda: up(array, 0, True).start())
        pl.when(level > 0)(lambda: down(array, 0, True).start())
        across(array, level, True).start()
    own_copies = [
        pltpu.make_async_copy(
            pairs[array][0],
            pairs[array][1].at[pl.ds(pl.multiple_of(me_y * depth, depth), depth), :],
            own_sem.at[array],
        )
        for array in (0, 1)
    ]
    for copy in own_copies:
        copy.start()
    keep_own(along.at[0], along.at[1], me_y, size_y)
    keep_own(along.at[0], along.at[2], me_z, size_z)
    for step in range(levels - 1):
        for array in (0, 1):

            @pl.when(level - 1 - step >= 0)
            def _():
                transfer(array, level - 1 - step, side, up_send, up_recv, step, above).wait_recv()
                pl.when(level + 1 < levels)(lambda: up(array, step + 1).start())
                across(array, level - 1 - step).start()
                share(array, level - 1 - step, side).start()

            @pl.when(level + 1 + step < levels)
            def _():
                transfer(array, level + 1 + step, side, down_send, down_recv, step, below).wait_recv()
                pl.when(level > 0)(lambda: down(array, step + 1).start())
                across(array, level + 1 + step).start()
                share(array, level + 1 + step, side).start()

    def finish(copy):
        copy.wait_send()
        copy.wait_recv()

    def arrived(array, lev):
        across_in = transfer(array, lev, 1 - side, side_send, side_recv, lev, beside)
        across_in.wait_recv()
        share(array, lev, 1 - side).start()

    for array in (0, 1):
        arrived(array, level)
    for step in range(1, levels):
        for array in (0, 1):
            pl.when(level - step >= 0)(lambda: arrived(array, level - step))
            pl.when(level + step < levels)(lambda: arrived(array, level + step))

    for copy in sent_y + sent_z + own_copies:
        copy.wait()
    for array in (0, 1):
        pl.when(level + 1 < levels)(lambda: up(array, 0, True).wait_send())
        pl.when(level > 0)(lambda: down(array, 0, True).wait_send())
        across(array, level, True).wait_send()
        finish(share(array, level, 1 - side))
        for step in range(1, levels):

            @pl.when(level - step >= 0)
            def _():
                pl.when(level + 1 < levels)(lambda: up(array, step).wait_send())
                across(array, level - step).wait_send()
                for sid in (side, 1 - side):
                    finish(share(array, level - step, sid))

            @pl.when(level + step < levels)
            def _():
                pl.when(level > 0)(lambda: down(array, step).wait_send())
                across(array, level + step).wait_send()
                for sid in (side, 1 - side):
                    finish(share(array, level + step, sid))


def line_places(rows, size_y, size_z, rows_z):
    row = np.arange(rows)
    part_y, part_z = rows // size_y, rows // size_z
    return (
        (row // rows_z, row % rows_z),
        (row // part_y, row % part_y),
        (row // part_z * rows_z + row % rows_z, row % part_z // rows_z),
    )


def offset_lookup(places, lengths, rows):
    parts, base = [], 0
    total = sum(2 * length - 1 for length in lengths)
    for (position, line), length in zip(places, lengths):
        lookup = np.zeros((total, 2 * rows), np.float32)
        first, second = np.nonzero(line[:, None] == line[None, :])
        entry = position[first] - position[second] + length - 1 + base
        lookup[entry, rows - 1 - first + second] = 1.0
        parts.append(lookup)
        base += 2 * length - 1
    return np.concatenate(parts, axis=1)


def attend_kernel(size_y, size_z, rows_z, heads, along, w_q, w_k, w_v, offsets, out):
    _, samples, rows, features = along.shape
    wide = w_q.shape[1]
    tokens = along[...].reshape(3 * samples * rows, features)

    def project(weights):
        return jnp.dot(tokens, weights[...], preferred_element_type=jnp.float32)

    query = (project(w_q) * HEAD ** (-0.5)).astype(jnp.bfloat16)
    keys = project(w_k).astype(jnp.bfloat16)
    values = project(w_v).astype(jnp.bfloat16)
    row = lax.broadcasted_iota(jnp.int32, (rows, rows), 0)
    col = lax.broadcasted_iota(jnp.int32, (rows, rows), 1)
    lane = lax.broadcasted_iota(jnp.int32, (rows, 2 * HEAD), 1)
    part_y, part_z = rows // size_y, rows // size_z
    line_of = (
        lambda r: lax.rem(r, rows_z),
        lambda r: lax.rem(r, part_y),
        lambda r: lax.rem(r, part_z) // rows_z,
    )
    for axis in range(3):
        same = line_of[axis](row) == line_of[axis](col)
        for pair in range(wide // (2 * HEAD)):
            columns = slice(pair * 2 * HEAD, (pair + 1) * 2 * HEAD)
            biases = []
            for half in range(2):
                entry = offsets[0, pair * 2 + half, axis * 2 * rows : (axis + 1) * 2 * rows]
                spread = jnp.broadcast_to(entry[None, :], (rows, 2 * rows))
                spread = pltpu.roll(spread, rows + 1, 1, stride=1, stride_axis=0)
                biases.append(jnp.where(same, spread[:, :rows], -1e30))
            for sample in range(samples):
                first = (axis * samples + sample) * rows
                part = slice(first, first + rows)
                mixed = []
                for half in range(2):
                    chosen = jnp.where(lane // HEAD == half, query[part, columns], 0)
                    scores = lax.dot_general(
                        chosen, keys[part, columns], (((1,), (1,)), ((), ())),
                        preferred_element_type=jnp.float32,
                    ) + biases[half]
                    expo = jnp.exp(scores - jnp.max(scores, axis=-1, keepdims=True))
                    weights = (expo / jnp.sum(expo, axis=-1, keepdims=True)).astype(jnp.bfloat16)
                    mixed.append(
                        jnp.dot(weights, values[part, columns], preferred_element_type=jnp.float32)
                    )
                out[axis, sample, :, columns] = jnp.where(lane < HEAD, mixed[0], mixed[1]).astype(
                    jnp.bfloat16
                )


def return_kernel(
    size_y, size_z, mixed, tokens, w_out, result, back_y, back_z, y_send, y_recv, z_send, z_recv
):
    me_y, me_z = lax.axis_index("gy"), lax.axis_index("gz")
    greet(me_y, me_z, size_y, size_z)
    copies = exchange(mixed.at[1], back_y, "gy", me_y, size_y, y_send, y_recv)
    copies += exchange(mixed.at[2], back_z, "gz", me_z, size_z, z_send, z_recv)
    keep_own(mixed.at[1], back_y, me_y, size_y)
    keep_own(mixed.at[2], back_z, me_z, size_z)
    for copy in copies:
        copy.wait()
    summed = mixed[0].astype(jnp.float32) + back_y[...].astype(jnp.float32)
    summed = (summed + back_z[...].astype(jnp.float32)).astype(jnp.bfloat16)
    summed = summed.reshape(-1, summed.shape[-1])
    width = 256
    for first in range(0, w_out.shape[1], width):
        columns = slice(first, first + width)
        product = jnp.dot(summed, w_out[:, columns], preferred_element_type=jnp.float32)
        residual = tokens[:, :, columns].astype(jnp.float32)
        result[:, :, columns] = (residual + product.reshape(residual.shape)).astype(jnp.bfloat16)


VMEM = pl.BlockSpec(memory_space=pltpu.VMEM)
ANY = pl.BlockSpec(memory_space=pl.ANY)
DMA = pltpu.SemaphoreType.DMA


def fast_shards(size_y, size_z, tokens, w_qkv, w_out, bias_x, bias_y, bias_z):
    samples, depth, rows_y, rows_z, features = tokens.shape
    rows = depth * rows_y * rows_z
    levels = size_y // 2
    lengths = [(table.shape[1] + 1) // 2 for table in (bias_x, bias_y, bias_z)]
    lookup = offset_lookup(line_places(rows, size_y, size_z, rows_z), lengths, rows)
    offsets = jnp.dot(
        jnp.concatenate([bias_x, bias_y, bias_z], axis=1), lookup, precision=lax.Precision.HIGHEST
    )
    flat = tokens.reshape(samples, rows, features)
    along, all_qkv, all_out = pl.pallas_call(
        functools.partial(gather_kernel, size_y, size_z),
        out_shape=(
            jax.ShapeDtypeStruct((3, samples, rows, features), jnp.bfloat16),
            jax.ShapeDtypeStruct((w_qkv.shape[0] * size_y, w_qkv.shape[1]), jnp.bfloat16),
            jax.ShapeDtypeStruct((w_out.shape[0] * size_y, w_out.shape[1]), jnp.bfloat16),
        ),
        in_specs=[VMEM, VMEM, VMEM],
        out_specs=(VMEM, ANY, ANY),
        scratch_shapes=[
            DMA((size_y - 1,)), DMA((size_y - 1,)), DMA((size_z - 1,)), DMA((size_z - 1,)),
            DMA((2, levels)), DMA((2, levels)), DMA((2, levels)), DMA((2, levels)),
            DMA((2, levels)), DMA((2, levels)), DMA((2, size_y)), DMA((2, size_y)), DMA((2,)),
        ],
        compiler_params=pltpu.CompilerParams(collective_id=0, has_side_effects=True),
    )(flat, w_qkv, w_out)
    wide = 4 * HEAD
    groups = features // wide
    mixed = pl.pallas_call(
        functools.partial(attend_kernel, size_y, size_z, rows_z, HEADS),
        out_shape=jax.ShapeDtypeStruct((3, samples, rows, features), jnp.bfloat16),
        grid=(groups,),
        in_specs=[
            pl.BlockSpec((3, samples, rows, features), lambda g: (0, 0, 0, 0)),
            pl.BlockSpec((features, wide), lambda g: (0, g)),
            pl.BlockSpec((features, wide), lambda g: (0, groups + g)),
            pl.BlockSpec((features, wide), lambda g: (0, 2 * groups + g)),
            pl.BlockSpec((1, 4, 6 * rows), lambda g: (g, 0, 0)),
        ],
        out_specs=pl.BlockSpec((3, samples, rows, wide), lambda g: (0, 0, 0, g)),
    )(along, all_qkv, all_qkv, all_qkv, offsets.reshape(groups, 4, 6 * rows))
    result = pl.pallas_call(
        functools.partial(return_kernel, size_y, size_z),
        out_shape=jax.ShapeDtypeStruct((samples, rows, features), jnp.bfloat16),
        in_specs=[VMEM, VMEM, VMEM],
        out_specs=VMEM,
        scratch_shapes=[
            pltpu.VMEM((samples, rows, features), jnp.bfloat16),
            pltpu.VMEM((samples, rows, features), jnp.bfloat16),
            DMA((size_y - 1,)), DMA((size_y - 1,)), DMA((size_z - 1,)), DMA((size_z - 1,)),
        ],
        compiler_params=pltpu.CompilerParams(collective_id=1, has_side_effects=True),
    )(mixed, flat, all_out)
    return result.reshape(tokens.shape)


def body_for(size_y, size_z):
    def body(tokens, *parameters):
        _, depth, rows_y, rows_z, features = tokens.shape
        rows = depth * rows_y * rows_z
        whole_parts = size_y % 2 == 0 and size_z % 2 == 0 and rows == 2 * HEAD
        if whole_parts and rows_y == 1 and rows % (16 * size_y) == 0 and rows % (16 * size_z) == 0:
            return fast_shards(size_y, size_z, tokens, *parameters)
        return shards(tokens, *parameters)

    return body


def solution(mesh):
    placed = (P(None, None, "gy", "gz", None), P("gy", None), P("gy", None), P(), P(), P())
    return jax.shard_map(
        body_for(mesh.shape["gy"], mesh.shape["gz"]),
        mesh=mesh,
        in_specs=placed,
        out_specs=P(None, None, "gy", "gz", None),
        check_vma=False,
    )
```

```python
import functools

import jax
import jax.numpy as jnp
import numpy as np
from jax import lax
from jax.experimental import pallas as pl
from jax.experimental.pallas import tpu as pltpu
from jax.sharding import PartitionSpec as P

HEADS = 16
HEAD = 64


einsum_forms = {
    1: ("bxyzhs,bwyzhs->byzhxw", "byzhxw,bwyzhs->bxyzhs"),
    2: ("bxyzhs,bxwzhs->bxzhyw", "bxzhyw,bxwzhs->bxyzhs"),
    3: ("bxyzhs,bxywhs->bxyhzw", "bxyhzw,bxywhs->bxyzhs"),
}


def norm_rows(tokens):
    values = tokens.astype(jnp.float32)
    center = jnp.mean(values, axis=-1, keepdims=True)
    spread = jnp.mean((values - center) ** 2, axis=-1, keepdims=True)
    return ((values - center) * lax.rsqrt(spread + 1e-05)).astype(jnp.bfloat16)


def rel_bias(table):
    length = (table.shape[1] + 1) // 2
    offsets = (
        lax.broadcasted_iota(jnp.int32, (length, length), 0)
        - lax.broadcasted_iota(jnp.int32, (length, length), 1)
        + length
        - 1
    )
    lookup = (
        offsets[:, :, None] == lax.broadcasted_iota(jnp.int32, (1, 1, 2 * length - 1), 2)
    ).astype(jnp.float32)
    return jnp.einsum("hr,ijr->hij", table, lookup, precision=lax.Precision.HIGHEST)


def attend(qkv, table, axis):
    dims = qkv.shape
    features = dims[-1] // 3
    parts = qkv.reshape(dims[:-1] + (3, HEADS, HEAD))
    query = parts[..., 0, :, :]
    keys = parts[..., 1, :, :]
    values = parts[..., 2, :, :]
    score_form, mix_form = einsum_forms[axis]
    scores = jnp.einsum(score_form, query, keys, preferred_element_type=jnp.float32) * HEAD ** (
        -0.5
    ) + rel_bias(table)
    scores = scores - jnp.max(scores, axis=-1, keepdims=True)
    expo = jnp.exp(scores)
    weights = (expo / jnp.sum(expo, axis=-1, keepdims=True)).astype(jnp.bfloat16)
    mixed = jnp.einsum(mix_form, weights, values, preferred_element_type=jnp.float32)
    return mixed.reshape(dims[:-1] + (features,)).astype(jnp.bfloat16)


def return_y(result):
    return lax.all_to_all(result, "gy", split_axis=2, concat_axis=1, tiled=True)


def return_z(result):
    return lax.all_to_all(result, "gz", split_axis=3, concat_axis=1, tiled=True)


def shards(tokens, w_qkv, w_out, bias_x, bias_y, bias_z):
    samples, depth, rows_y, rows_z, features = tokens.shape
    normed = norm_rows(tokens)
    gathered = lax.all_gather(w_qkv, "gy", axis=0, tiled=True)

    def project(inputs):
        product = jnp.dot(
            inputs.reshape(-1, features), gathered, preferred_element_type=jnp.float32
        )
        return product.astype(jnp.bfloat16).reshape(inputs.shape[:-1] + (3 * features,))

    along_x = attend(project(normed), bias_x, 1)
    along_y = return_y(
        attend(
            project(lax.all_to_all(normed, "gy", split_axis=1, concat_axis=2, tiled=True)),
            bias_y,
            2,
        )
    )
    along_z = return_z(
        attend(
            project(lax.all_to_all(normed, "gz", split_axis=1, concat_axis=3, tiled=True)),
            bias_z,
            3,
        )
    )
    summed = along_x.astype(jnp.float32) + along_y.astype(jnp.float32) + along_z.astype(jnp.float32)
    summed = summed.astype(jnp.bfloat16).reshape(-1, features)
    residual = tokens.reshape(-1, features).astype(jnp.float32)
    result = residual + jnp.dot(
        summed, lax.all_gather(w_out, "gy", axis=0, tiled=True), preferred_element_type=jnp.float32
    )
    return result.astype(jnp.bfloat16).reshape(tokens.shape)


def device(**where):
    return {"device_id": where, "device_id_type": pl.DeviceIdType.MESH}


def greet(me_y, me_z, size_y, size_z):
    barrier = pltpu.get_barrier_semaphore()
    for step in range(1, size_y):
        pl.semaphore_signal(barrier, inc=1, **device(gy=lax.rem(me_y + step, size_y)))
    for step in range(1, size_z):
        pl.semaphore_signal(barrier, inc=1, **device(gz=lax.rem(me_z + step, size_z)))
    pl.semaphore_wait(barrier, size_y + size_z - 2)


def exchange(source, target, axis, me, size, send_sems, recv_sems):
    rows = source.shape[1] // size
    copies = []
    for step in range(1, size):
        peer = lax.rem(me + step, size)
        copies.append(
            pltpu.make_async_remote_copy(
                src_ref=source.at[:, pl.ds(pl.multiple_of(peer * rows, rows), rows), :],
                dst_ref=target.at[:, pl.ds(pl.multiple_of(me * rows, rows), rows), :],
                send_sem=send_sems.at[step - 1],
                recv_sem=recv_sems.at[step - 1],
                **device(**{axis: peer}),
            )
        )
    for copy in copies:
        copy.start()
    return copies


def keep_own(source, target, me, size):
    rows = source.shape[1] // size
    own = pl.ds(pl.multiple_of(me * rows, rows), rows)
    target[:, own, :] = source[:, own, :]


def line_places(rows, size_y, size_z, rows_z):
    row = np.arange(rows)
    part_y, part_z = rows // size_y, rows // size_z
    return (
        (row // rows_z, row % rows_z),
        (row // part_y, row % part_y),
        (row // part_z * rows_z + row % rows_z, row % part_z // rows_z),
    )


def offset_lookup(places, lengths, rows):
    parts, base = [], 0
    total = sum(2 * length - 1 for length in lengths)
    for (position, line), length in zip(places, lengths):
        lookup = np.zeros((total, 2 * rows), np.float32)
        first, second = np.nonzero(line[:, None] == line[None, :])
        entry = position[first] - position[second] + length - 1 + base
        lookup[entry, rows - 1 - first + second] = 1.0
        parts.append(lookup)
        base += 2 * length - 1
    return np.concatenate(parts, axis=1)


def fused_kernel(
    size_y, size_z, rows_z, tokens, weights, offsets, result,
    along, full, biases, mixed, back_y, back_z,
    y_send, y_recv, z_send, z_recv, up_send, up_recv, down_send, down_recv,
    side_send, side_recv, far_send, far_recv, core_send, core_recv, twin_send, twin_recv,
    ry_send, ry_recv, rz_send, rz_recv,
):
    me_y, me_z = lax.axis_index("gy"), lax.axis_index("gz")
    samples, rows, features = tokens.shape
    depth = weights.shape[1]
    half = depth // 2
    quarter = half // 4
    levels = size_y // 2
    wide = 4 * HEAD
    groups = features // wide
    level, side, core = me_y // 2, lax.rem(me_y, 2), lax.rem(me_z, 2)
    flank = lax.rem(me_z // 2, 2)
    above, below = {"gy": me_y + 2}, {"gy": me_y - 2}
    beside = {"gy": level * 2 + 1 - side}
    twin = {"gz": me_z + 1 - 2 * core}
    far = {"gz": me_z + 2 - 4 * flank}

    values = tokens[...].astype(jnp.float32)
    center = jnp.mean(values, axis=-1, keepdims=True)
    spread = jnp.mean((values - center) ** 2, axis=-1, keepdims=True)
    along[0] = ((values - center) * lax.rsqrt(spread + 1e-05)).astype(jnp.bfloat16)

    greet(me_y, me_z, size_y, size_z)

    def columns_of(group):
        return pl.ds(pl.multiple_of(group * wide, wide), wide)

    def transfer(group, lev, sid, start, count, sends, recvs, slot, where, own=False):
        first = core * half + start
        cols = columns_of(group)
        block = full.at[
            :, pl.ds(pl.multiple_of((lev * 2 + sid) * depth + first, quarter), count), cols
        ]
        source = block
        if own:
            source = weights.at[:, pl.ds(pl.multiple_of(first, quarter), count), cols]
        return pltpu.make_async_remote_copy(
            src_ref=source, dst_ref=block, send_sem=sends.at[group, slot],
            recv_sem=recvs.at[group, slot], **device(**where),
        )

    mine, held = flank * quarter, 3 * quarter

    def up(group, step, own=False):
        return transfer(group, level - step, side, mine, held, up_send, up_recv, step, above, own)

    def up_in(group, step):
        return transfer(group, level - 1 - step, side, mine, held, up_send, up_recv, step, above)

    def down(group, step, own=False):
        return transfer(group, level + step, side, mine, held, down_send, down_recv, step, below, own)

    def down_in(group, step):
        return transfer(group, level + 1 + step, side, mine, held, down_send, down_recv, step, below)

    def across(group, lev, own=False):
        return transfer(group, lev, side, mine, held, side_send, side_recv, lev, beside, own)

    def across_in(group, lev):
        return transfer(group, lev, 1 - side, mine, held, side_send, side_recv, lev, beside)

    def share(group, lev, sid):
        return transfer(
            group, lev, sid, mine, held, core_send, core_recv, lev * 2 + sid, twin
        )

    def to_far(group, lev, sid):
        return transfer(
            group, lev, sid, flank * 3 * quarter, quarter, far_send, far_recv, lev * 2 + sid, far
        )

    def share_far(group, lev, sid):
        return transfer(
            group, lev, sid, (1 - flank) * 3 * quarter, quarter,
            twin_send, twin_recv, lev * 2 + sid, twin,
        )

    def own_blocks(group):
        pl.when(level + 1 < levels)(lambda: up(group, 0, True).start())
        pl.when(level > 0)(lambda: down(group, 0, True).start())
        across(group, level, True).start()

    def spread_block(group, lev, sid):
        to_far(group, lev, sid).start()
        share(group, lev, sid).start()

    def chain(group, step):
        @pl.when(level - 1 - step >= 0)
        def _():
            up_in(group, step).wait_recv()
            pl.when(level + 1 < levels)(lambda: up(group, step + 1).start())
            across(group, level - 1 - step).start()
            spread_block(group, level - 1 - step, side)

        @pl.when(level + 1 + step < levels)
        def _():
            down_in(group, step).wait_recv()
            pl.when(level > 0)(lambda: down(group, step + 1).start())
            across(group, level + 1 + step).start()
            spread_block(group, level + 1 + step, side)

    def from_side(group, step):
        def arrived(lev):
            across_in(group, lev).wait_recv()
            spread_block(group, lev, 1 - side)

        if step == 0:
            arrived(level)
        else:
            pl.when(level - step >= 0)(lambda: arrived(level - step))
            pl.when(level + step < levels)(lambda: arrived(level + step))

    def each_block(act):
        act(level, 1 - side)
        for step in range(1, levels):
            for lev, there in ((level - step, level - step >= 0), (level + step, level + step < levels)):

                @pl.when(there)
                def _():
                    act(lev, side)
                    act(lev, 1 - side)

    def from_far(group):
        def act(lev, sid):
            to_far_in = transfer(
                group, lev, sid, (1 - flank) * 3 * quarter, quarter,
                far_send, far_recv, lev * 2 + sid, far,
            )
            to_far_in.wait_recv()
            share_far(group, lev, sid).start()

        each_block(act)

    def complete(group):
        def act(lev, sid):
            transfer(
                group, lev, sid, mine, held, core_send, core_recv, lev * 2 + sid, twin
            ).wait_recv()
            share_far(group, lev, sid).wait_recv()

        each_block(act)

    def drain(group):
        pl.when(level + 1 < levels)(lambda: up(group, 0, True).wait_send())
        pl.when(level > 0)(lambda: down(group, 0, True).wait_send())
        across(group, level, True).wait_send()
        for step in range(1, levels):

            @pl.when(level - step >= 0)
            def _():
                pl.when(level + 1 < levels)(lambda: up(group, step).wait_send())
                across(group, level - step).wait_send()

            @pl.when(level + step < levels)
            def _():
                pl.when(level > 0)(lambda: down(group, step).wait_send())
                across(group, level + step).wait_send()

        def act(lev, sid):
            to_far(group, lev, sid).wait_send()
            share(group, lev, sid).wait_send()
            share_far(group, lev, sid).wait_send()

        each_block(act)

    own_blocks(0)
    sent_y = exchange(along.at[0], along.at[1], "gy", me_y, size_y, y_send, y_recv)
    sent_z = exchange(along.at[0], along.at[2], "gz", me_z, size_z, z_send, z_recv)
    own_blocks(1)
    full[:, pl.ds(pl.multiple_of(me_y * depth, depth), depth), :] = weights[...]
    keep_own(along.at[0], along.at[1], me_y, size_y)
    keep_own(along.at[0], along.at[2], me_z, size_z)

    for step in range(levels - 1):
        chain(0, step)

    row = lax.broadcasted_iota(jnp.int32, (rows, rows), 0)
    col = lax.broadcasted_iota(jnp.int32, (rows, rows), 1)
    lane = lax.broadcasted_iota(jnp.int32, (rows, 2 * HEAD), 1)
    part_y, part_z = rows // size_y, rows // size_z
    line_of = (
        lambda r: lax.rem(r, rows_z),
        lambda r: lax.rem(r, part_y),
        lambda r: lax.rem(r, part_z) // rows_z,
    )

    def fill_bias(group, carry):
        for axis in range(3):
            same = line_of[axis](row) == line_of[axis](col)
            for head in range(4):
                entry = offsets[group, head, axis * 2 * rows : (axis + 1) * 2 * rows]
                table = jnp.broadcast_to(entry[None, :], (rows, 2 * rows))
                table = pltpu.roll(table, rows + 1, 1, stride=1, stride_axis=0)
                biases[axis, group * 4 + head] = jnp.where(same, table[:, :rows], -1e30)
        return carry

    lax.fori_loop(0, groups, fill_bias, 0)

    for step in range(levels):
        from_side(0, step)
    for copy in sent_y + sent_z:
        copy.wait()
    from_far(0)
    complete(0)

    def attend(group, axis, pair, query, keys, contents):
        cols = slice(pair * 2 * HEAD, (pair + 1) * 2 * HEAD)
        for sample in range(samples):
            first = (axis * samples + sample) * rows
            part = slice(first, first + rows)
            outs = []
            for odd in range(2):
                chosen = jnp.where(lane // HEAD == odd, query[part, cols], 0)
                scores = lax.dot_general(
                    chosen, keys[part, cols], (((1,), (1,)), ((), ())),
                    preferred_element_type=jnp.float32,
                ) + biases[axis, group * 4 + pair * 2 + odd]
                expo = jnp.exp(scores - jnp.max(scores, axis=-1, keepdims=True))
                scale = 1.0 / jnp.sum(expo, axis=-1, keepdims=True)
                outs.append(
                    jnp.dot(
                        (expo * scale).astype(jnp.bfloat16), contents[part, cols],
                        preferred_element_type=jnp.float32,
                    )
                )
            place = pl.ds(pl.multiple_of(group * wide + pair * 2 * HEAD, 2 * HEAD), 2 * HEAD)
            mixed[axis, sample, :, place] = jnp.where(lane < HEAD, outs[0], outs[1]).astype(
                jnp.bfloat16
            )

    def returns(group):
        cols = columns_of(group)
        there = [
            (mixed.at[1], back_y, "gy", me_y, size_y, ry_send, ry_recv),
            (mixed.at[2], back_z, "gz", me_z, size_z, rz_send, rz_recv),
        ]
        copies = []
        for source, target, axis, me, size, sends, recvs in there:
            count = rows // size
            for step in range(1, size):
                peer = lax.rem(me + step, size)
                copies.append(
                    pltpu.make_async_remote_copy(
                        src_ref=source.at[:, pl.ds(pl.multiple_of(peer * count, count), count), cols],
                        dst_ref=target.at[:, pl.ds(pl.multiple_of(me * count, count), count), cols],
                        send_sem=sends.at[group, step - 1],
                        recv_sem=recvs.at[group, step - 1],
                        **device(**{axis: peer}),
                    )
                )
        return copies

    def group_step(group, carry):
        ahead = group + 1
        more = ahead < groups
        flat = along[...].reshape(3 * samples * rows, features)
        cols = columns_of(group)

        def project(which):
            return jnp.dot(flat, full[which, :, cols], preferred_element_type=jnp.float32)

        pl.when(more)(lambda: chain(ahead, 0))
        query = (project(0) * HEAD ** (-0.5)).astype(jnp.bfloat16)
        keys = project(1).astype(jnp.bfloat16)
        contents = project(2).astype(jnp.bfloat16)
        pl.when(ahead + 1 < groups)(lambda: own_blocks(ahead + 1))
        pending = [functools.partial(chain, ahead, step) for step in range(1, levels - 1)]
        pending += [functools.partial(from_side, ahead, step) for step in range(levels)]
        pieces = [(axis, pair) for axis in (1, 2, 0) for pair in range(wide // (2 * HEAD))]
        for number, (axis, pair) in enumerate(pieces):
            attend(group, axis, pair, query, keys, contents)
            if number < len(pending):
                now = [pending[number]] if number + 1 < len(pieces) else pending[number:]

                @pl.when(more)
                def _():
                    for act in now:
                        act()

        for copy in returns(group):
            copy.start()

        @pl.when(more)
        def _():
            from_far(ahead)
            complete(ahead)

        return carry

    lax.fori_loop(0, groups, group_step, 0)
    keep_own(mixed.at[1], back_y, me_y, size_y)
    keep_own(mixed.at[2], back_z, me_z, size_z)

    def finish(group, carry):
        drain(group)
        for copy in returns(group):
            copy.wait()
        return carry

    lax.fori_loop(0, groups, finish, 0)
    summed = mixed[0].astype(jnp.float32) + back_y[...].astype(jnp.float32)
    summed = (summed + back_z[...].astype(jnp.float32)).astype(jnp.bfloat16)
    summed = summed.reshape(-1, features)
    for first in range(0, features, wide):
        cols = slice(first, first + wide)
        product = jnp.dot(summed, full[3, :, cols], preferred_element_type=jnp.float32)
        residual = tokens[:, :, cols].astype(jnp.float32)
        result[:, :, cols] = (residual + product.reshape(residual.shape)).astype(jnp.bfloat16)


VMEM = pl.BlockSpec(memory_space=pltpu.VMEM)
DMA = pltpu.SemaphoreType.DMA


def fast_shards(size_y, size_z, tokens, w_qkv, w_out, bias_x, bias_y, bias_z):
    samples, depth, rows_y, rows_z, features = tokens.shape
    rows = depth * rows_y * rows_z
    levels = size_y // 2
    groups = features // (4 * HEAD)
    lengths = [(table.shape[1] + 1) // 2 for table in (bias_x, bias_y, bias_z)]
    lookup = offset_lookup(line_places(rows, size_y, size_z, rows_z), lengths, rows)
    offsets = jnp.dot(
        jnp.concatenate([bias_x, bias_y, bias_z], axis=1), lookup, precision=lax.Precision.HIGHEST
    )
    weights = jnp.stack([w_qkv[:, n * features : (n + 1) * features] for n in range(3)] + [w_out])
    block = (samples, rows, features)
    result = pl.pallas_call(
        functools.partial(fused_kernel, size_y, size_z, rows_z),
        out_shape=jax.ShapeDtypeStruct(block, jnp.bfloat16),
        in_specs=[VMEM, VMEM, VMEM],
        out_specs=VMEM,
        scratch_shapes=[
            pltpu.VMEM((3,) + block, jnp.bfloat16),
            pltpu.VMEM((4, features, features), jnp.bfloat16),
            pltpu.VMEM((3, HEADS, rows, rows), jnp.float32),
            pltpu.VMEM((3,) + block, jnp.bfloat16),
            pltpu.VMEM(block, jnp.bfloat16),
            pltpu.VMEM(block, jnp.bfloat16),
            DMA((size_y - 1,)), DMA((size_y - 1,)), DMA((size_z - 1,)), DMA((size_z - 1,)),
            DMA((groups, levels)), DMA((groups, levels)), DMA((groups, levels)), DMA((groups, levels)),
            DMA((groups, levels)), DMA((groups, levels)),
            DMA((groups, size_y)), DMA((groups, size_y)),
            DMA((groups, size_y)), DMA((groups, size_y)),
            DMA((groups, size_y)), DMA((groups, size_y)),
            DMA((groups, size_y - 1)), DMA((groups, size_y - 1)),
            DMA((groups, size_z - 1)), DMA((groups, size_z - 1)),
        ],
        compiler_params=pltpu.CompilerParams(collective_id=0, has_side_effects=True),
    )(tokens.reshape(block), weights, offsets.reshape(groups, 4, 6 * rows))
    return result.reshape(tokens.shape)


def body_for(size_y, size_z):
    def body(tokens, *parameters):
        _, depth, rows_y, rows_z, features = tokens.shape
        rows = depth * rows_y * rows_z
        whole_parts = size_y % 2 == 0 and size_z % 4 == 0 and rows == 2 * HEAD
        if whole_parts and rows_y == 1 and rows % (16 * size_y) == 0 and rows % (16 * size_z) == 0:
            return fast_shards(size_y, size_z, tokens, *parameters)
        return shards(tokens, *parameters)

    return body


def solution(mesh):
    placed = (P(None, None, "gy", "gz", None), P("gy", None), P("gy", None), P(), P(), P())
    return jax.shard_map(
        body_for(mesh.shape["gy"], mesh.shape["gz"]),
        mesh=mesh,
        in_specs=placed,
        out_specs=P(None, None, "gy", "gz", None),
        check_vma=False,
    )
```

```python
import functools

import jax
import jax.numpy as jnp
import numpy as np
from jax import lax
from jax.experimental import pallas as pl
from jax.experimental.pallas import tpu as pltpu
from jax.sharding import PartitionSpec as P

HEADS = 16
HEAD = 64


einsum_forms = {
    1: ("bxyzhs,bwyzhs->byzhxw", "byzhxw,bwyzhs->bxyzhs"),
    2: ("bxyzhs,bxwzhs->bxzhyw", "bxzhyw,bxwzhs->bxyzhs"),
    3: ("bxyzhs,bxywhs->bxyhzw", "bxyhzw,bxywhs->bxyzhs"),
}


def norm_rows(tokens):
    values = tokens.astype(jnp.float32)
    center = jnp.mean(values, axis=-1, keepdims=True)
    spread = jnp.mean((values - center) ** 2, axis=-1, keepdims=True)
    return ((values - center) * lax.rsqrt(spread + 1e-05)).astype(jnp.bfloat16)


def rel_bias(table):
    length = (table.shape[1] + 1) // 2
    offsets = (
        lax.broadcasted_iota(jnp.int32, (length, length), 0)
        - lax.broadcasted_iota(jnp.int32, (length, length), 1)
        + length
        - 1
    )
    lookup = (
        offsets[:, :, None] == lax.broadcasted_iota(jnp.int32, (1, 1, 2 * length - 1), 2)
    ).astype(jnp.float32)
    return jnp.einsum("hr,ijr->hij", table, lookup, precision=lax.Precision.HIGHEST)


def attend(qkv, table, axis):
    dims = qkv.shape
    features = dims[-1] // 3
    parts = qkv.reshape(dims[:-1] + (3, HEADS, HEAD))
    query = parts[..., 0, :, :]
    keys = parts[..., 1, :, :]
    values = parts[..., 2, :, :]
    score_form, mix_form = einsum_forms[axis]
    scores = jnp.einsum(score_form, query, keys, preferred_element_type=jnp.float32) * HEAD ** (
        -0.5
    ) + rel_bias(table)
    scores = scores - jnp.max(scores, axis=-1, keepdims=True)
    expo = jnp.exp(scores)
    weights = (expo / jnp.sum(expo, axis=-1, keepdims=True)).astype(jnp.bfloat16)
    mixed = jnp.einsum(mix_form, weights, values, preferred_element_type=jnp.float32)
    return mixed.reshape(dims[:-1] + (features,)).astype(jnp.bfloat16)


def return_y(result):
    return lax.all_to_all(result, "gy", split_axis=2, concat_axis=1, tiled=True)


def return_z(result):
    return lax.all_to_all(result, "gz", split_axis=3, concat_axis=1, tiled=True)


def shards(tokens, w_qkv, w_out, bias_x, bias_y, bias_z):
    samples, depth, rows_y, rows_z, features = tokens.shape
    normed = norm_rows(tokens)
    gathered = lax.all_gather(w_qkv, "gy", axis=0, tiled=True)

    def project(inputs):
        product = jnp.dot(
            inputs.reshape(-1, features), gathered, preferred_element_type=jnp.float32
        )
        return product.astype(jnp.bfloat16).reshape(inputs.shape[:-1] + (3 * features,))

    along_x = attend(project(normed), bias_x, 1)
    along_y = return_y(
        attend(
            project(lax.all_to_all(normed, "gy", split_axis=1, concat_axis=2, tiled=True)),
            bias_y,
            2,
        )
    )
    along_z = return_z(
        attend(
            project(lax.all_to_all(normed, "gz", split_axis=1, concat_axis=3, tiled=True)),
            bias_z,
            3,
        )
    )
    summed = along_x.astype(jnp.float32) + along_y.astype(jnp.float32) + along_z.astype(jnp.float32)
    summed = summed.astype(jnp.bfloat16).reshape(-1, features)
    residual = tokens.reshape(-1, features).astype(jnp.float32)
    result = residual + jnp.dot(
        summed, lax.all_gather(w_out, "gy", axis=0, tiled=True), preferred_element_type=jnp.float32
    )
    return result.astype(jnp.bfloat16).reshape(tokens.shape)


def device(**where):
    return {"device_id": where, "device_id_type": pl.DeviceIdType.MESH}


def greet(me_y, me_z, size_y, size_z):
    barrier = pltpu.get_barrier_semaphore()
    for step in range(1, size_y):
        pl.semaphore_signal(barrier, inc=1, **device(gy=lax.rem(me_y + step, size_y)))
    for step in range(1, size_z):
        pl.semaphore_signal(barrier, inc=1, **device(gz=lax.rem(me_z + step, size_z)))
    pl.semaphore_wait(barrier, size_y + size_z - 2)


def exchange(source, target, axis, me, size, send_sems, recv_sems):
    rows = source.shape[1] // size
    copies = []
    for step in range(1, size):
        peer = lax.rem(me + step, size)
        copies.append(
            pltpu.make_async_remote_copy(
                src_ref=source.at[:, pl.ds(pl.multiple_of(peer * rows, rows), rows), :],
                dst_ref=target.at[:, pl.ds(pl.multiple_of(me * rows, rows), rows), :],
                send_sem=send_sems.at[step - 1],
                recv_sem=recv_sems.at[step - 1],
                **device(**{axis: peer}),
            )
        )
    for copy in copies:
        copy.start()
    return copies


def keep_own(source, target, me, size):
    rows = source.shape[1] // size
    own = pl.ds(pl.multiple_of(me * rows, rows), rows)
    target[:, own, :] = source[:, own, :]


def line_places(rows, size_y, size_z, rows_z):
    row = np.arange(rows)
    part_y, part_z = rows // size_y, rows // size_z
    return (
        (row // rows_z, row % rows_z),
        (row // part_y, row % part_y),
        (row // part_z * rows_z + row % rows_z, row % part_z // rows_z),
    )


def offset_lookup(places, lengths, rows):
    parts, base = [], 0
    total = sum(2 * length - 1 for length in lengths)
    for (position, line), length in zip(places, lengths):
        lookup = np.zeros((total, 2 * rows), np.float32)
        first, second = np.nonzero(line[:, None] == line[None, :])
        entry = position[first] - position[second] + length - 1 + base
        lookup[entry, rows - 1 - first + second] = 1.0
        parts.append(lookup)
        base += 2 * length - 1
    return np.concatenate(parts, axis=1)


def fused_kernel(
    size_y, size_z, rows_z, tokens, weights, offsets, result,
    along, full, biases, mixed, back_y, back_z,
    y_send, y_recv, z_send, z_recv, up_send, up_recv, down_send, down_recv,
    side_send, side_recv, far_send, far_recv, core_send, core_recv, twin_send, twin_recv,
    ry_send, ry_recv, rz_send, rz_recv,
):
    me_y, me_z = lax.axis_index("gy"), lax.axis_index("gz")
    samples, rows, features = tokens.shape
    depth = weights.shape[1]
    half = depth // 2
    quarter = half // 4
    levels = size_y // 2
    wide = 4 * HEAD
    groups = features // wide
    level, side, core = me_y // 2, lax.rem(me_y, 2), lax.rem(me_z, 2)
    flank = lax.rem(me_z // 2, 2)
    above, below = {"gy": me_y + 2}, {"gy": me_y - 2}
    beside = {"gy": level * 2 + 1 - side}
    twin = {"gz": me_z + 1 - 2 * core}
    far = {"gz": me_z + 2 - 4 * flank}

    values = tokens[...].astype(jnp.float32)
    center = jnp.mean(values, axis=-1, keepdims=True)
    spread = jnp.mean((values - center) ** 2, axis=-1, keepdims=True)
    along[0] = ((values - center) * lax.rsqrt(spread + 1e-05)).astype(jnp.bfloat16)

    greet(me_y, me_z, size_y, size_z)

    def columns_of(group):
        return pl.ds(pl.multiple_of(group * wide, wide), wide)

    def transfer(group, lev, sid, start, count, sends, recvs, slot, where, own=False):
        first = core * half + start
        cols = columns_of(group)
        block = full.at[
            :, pl.ds(pl.multiple_of((lev * 2 + sid) * depth + first, quarter), count), cols
        ]
        source = block
        if own:
            source = weights.at[:, pl.ds(pl.multiple_of(first, quarter), count), cols]
        return pltpu.make_async_remote_copy(
            src_ref=source, dst_ref=block, send_sem=sends.at[group, slot],
            recv_sem=recvs.at[group, slot], **device(**where),
        )

    mine, held = flank * quarter, 3 * quarter

    def up(group, step, own=False):
        return transfer(group, level - step, side, mine, held, up_send, up_recv, step, above, own)

    def up_in(group, step):
        return transfer(group, level - 1 - step, side, mine, held, up_send, up_recv, step, above)

    def down(group, step, own=False):
        return transfer(group, level + step, side, mine, held, down_send, down_recv, step, below, own)

    def down_in(group, step):
        return transfer(group, level + 1 + step, side, mine, held, down_send, down_recv, step, below)

    def across(group, lev, own=False):
        return transfer(group, lev, side, mine, held, side_send, side_recv, lev, beside, own)

    def across_in(group, lev):
        return transfer(group, lev, 1 - side, mine, held, side_send, side_recv, lev, beside)

    def share(group, lev, sid):
        return transfer(
            group, lev, sid, mine, held, core_send, core_recv, lev * 2 + sid, twin
        )

    def to_far(group, lev, sid):
        return transfer(
            group, lev, sid, flank * 3 * quarter, quarter, far_send, far_recv, lev * 2 + sid, far
        )

    def share_far(group, lev, sid):
        return transfer(
            group, lev, sid, (1 - flank) * 3 * quarter, quarter,
            twin_send, twin_recv, lev * 2 + sid, twin,
        )

    def own_blocks(group):
        pl.when(level + 1 < levels)(lambda: up(group, 0, True).start())
        pl.when(level > 0)(lambda: down(group, 0, True).start())
        across(group, level, True).start()

    def spread_block(group, lev, sid):
        to_far(group, lev, sid).start()
        share(group, lev, sid).start()

    def chain(group, step):
        @pl.when(level - 1 - step >= 0)
        def _():
            up_in(group, step).wait_recv()
            pl.when(level + 1 < levels)(lambda: up(group, step + 1).start())
            across(group, level - 1 - step).start()
            spread_block(group, level - 1 - step, side)

        @pl.when(level + 1 + step < levels)
        def _():
            down_in(group, step).wait_recv()
            pl.when(level > 0)(lambda: down(group, step + 1).start())
            across(group, level + 1 + step).start()
            spread_block(group, level + 1 + step, side)

    def from_side(group, step):
        def arrived(lev):
            across_in(group, lev).wait_recv()
            spread_block(group, lev, 1 - side)

        if step == 0:
            arrived(level)
        else:
            pl.when(level - step >= 0)(lambda: arrived(level - step))
            pl.when(level + step < levels)(lambda: arrived(level + step))

    def each_block(act):
        act(level, 1 - side)
        for step in range(1, levels):
            for lev, there in ((level - step, level - step >= 0), (level + step, level + step < levels)):

                @pl.when(there)
                def _():
                    act(lev, side)
                    act(lev, 1 - side)

    def from_far(group):
        def act(lev, sid):
            to_far_in = transfer(
                group, lev, sid, (1 - flank) * 3 * quarter, quarter,
                far_send, far_recv, lev * 2 + sid, far,
            )
            to_far_in.wait_recv()
            share_far(group, lev, sid).start()

        each_block(act)

    def complete(group):
        def act(lev, sid):
            transfer(
                group, lev, sid, mine, held, core_send, core_recv, lev * 2 + sid, twin
            ).wait_recv()
            share_far(group, lev, sid).wait_recv()

        each_block(act)

    def drain(group):
        pl.when(level + 1 < levels)(lambda: up(group, 0, True).wait_send())
        pl.when(level > 0)(lambda: down(group, 0, True).wait_send())
        across(group, level, True).wait_send()
        for step in range(1, levels):

            @pl.when(level - step >= 0)
            def _():
                pl.when(level + 1 < levels)(lambda: up(group, step).wait_send())
                across(group, level - step).wait_send()

            @pl.when(level + step < levels)
            def _():
                pl.when(level > 0)(lambda: down(group, step).wait_send())
                across(group, level + step).wait_send()

        def act(lev, sid):
            to_far(group, lev, sid).wait_send()
            share(group, lev, sid).wait_send()
            share_far(group, lev, sid).wait_send()

        each_block(act)

    own_blocks(0)
    sent_y = exchange(along.at[0], along.at[1], "gy", me_y, size_y, y_send, y_recv)
    sent_z = exchange(along.at[0], along.at[2], "gz", me_z, size_z, z_send, z_recv)
    for group in range(1, groups):
        own_blocks(group)
    full[:, pl.ds(pl.multiple_of(me_y * depth, depth), depth), :] = weights[...]
    keep_own(along.at[0], along.at[1], me_y, size_y)
    keep_own(along.at[0], along.at[2], me_z, size_z)

    row = lax.broadcasted_iota(jnp.int32, (rows, rows), 0)
    col = lax.broadcasted_iota(jnp.int32, (rows, rows), 1)
    lane = lax.broadcasted_iota(jnp.int32, (rows, 2 * HEAD), 1)
    part_y, part_z = rows // size_y, rows // size_z
    line_of = (
        lambda r: lax.rem(r, rows_z),
        lambda r: lax.rem(r, part_y),
        lambda r: lax.rem(r, part_z) // rows_z,
    )

    def fill_bias(group, carry):
        for axis in range(3):
            same = line_of[axis](row) == line_of[axis](col)
            for head in range(4):
                entry = offsets[group, head, axis * 2 * rows : (axis + 1) * 2 * rows]
                table = jnp.broadcast_to(entry[None, :], (rows, 2 * rows))
                table = pltpu.roll(table, rows + 1, 1, stride=1, stride_axis=0)
                biases[axis, group * 4 + head] = jnp.where(same, table[:, :rows], -1e30)
        return carry

    lax.fori_loop(0, groups, fill_bias, 0)

    hops = levels - 1
    waves = [
        [(wave - step, step) for step in range(hops) if 0 <= wave - step < groups]
        for wave in range(groups + hops - 1)
    ]

    def run(chosen):
        for wave in chosen:
            for group, step in wave:
                chain(group, step)

    run(waves[:hops])
    for step in range(levels):
        from_side(0, step)
    run(waves[hops : hops + 1])
    from_far(0)
    if groups > 1:
        for step in range(levels):
            from_side(1, step)
    run(waves[hops + 1 : -1])
    for copy in sent_y + sent_z:
        copy.wait()
    complete(0)

    def attend(group, axis, query, keys, contents):
        units = [
            (pair, sample, odd)
            for pair in range(wide // (2 * HEAD)) for sample in range(samples) for odd in range(2)
        ]

        def parts(pair, sample):
            first = (axis * samples + sample) * rows
            return slice(first, first + rows), slice(pair * 2 * HEAD, (pair + 1) * 2 * HEAD)

        scores, expos, totals, outs = {}, {}, {}, {}
        for unit in units:
            pair, sample, odd = unit
            part = parts(pair, sample)
            chosen = jnp.where(lane // HEAD == odd, query[part], 0)
            scores[unit] = lax.dot_general(
                chosen, keys[part], (((1,), (1,)), ((), ())), preferred_element_type=jnp.float32
            ) + biases[axis, group * 4 + pair * 2 + odd]
        for unit in units:
            expos[unit] = jnp.exp(scores[unit] - jnp.max(scores[unit], axis=-1, keepdims=True))
            totals[unit] = jnp.sum(expos[unit], axis=-1, keepdims=True)
        for unit in units:
            outs[unit] = jnp.dot(
                expos[unit].astype(jnp.bfloat16), contents[parts(*unit[:2])],
                preferred_element_type=jnp.float32,
            )
        for pair, sample, odd in units[::2]:
            place = pl.ds(pl.multiple_of(group * wide + pair * 2 * HEAD, 2 * HEAD), 2 * HEAD)
            even, other = (pair, sample, 0), (pair, sample, 1)
            mixed[axis, sample, :, place] = jnp.where(
                lane < HEAD, outs[even] * (1.0 / totals[even]), outs[other] * (1.0 / totals[other])
            ).astype(jnp.bfloat16)

    def returns(group):
        cols = columns_of(group)
        there = [
            (mixed.at[1], back_y, "gy", me_y, size_y, ry_send, ry_recv),
            (mixed.at[2], back_z, "gz", me_z, size_z, rz_send, rz_recv),
        ]
        copies = []
        for source, target, axis, me, size, sends, recvs in there:
            count = rows // size
            for step in range(1, size):
                peer = lax.rem(me + step, size)
                copies.append(
                    pltpu.make_async_remote_copy(
                        src_ref=source.at[:, pl.ds(pl.multiple_of(peer * count, count), count), cols],
                        dst_ref=target.at[:, pl.ds(pl.multiple_of(me * count, count), count), cols],
                        send_sem=sends.at[group, step - 1],
                        recv_sem=recvs.at[group, step - 1],
                        **device(**{axis: peer}),
                    )
                )
        return copies

    def group_step(group, carry):
        ahead, later = group + 1, group + 2
        flat = along[...].reshape(3 * samples * rows, features)
        cols = columns_of(group)

        def project(which):
            return jnp.dot(flat, full[which, :, cols], preferred_element_type=jnp.float32)

        def bring(chosen):
            @pl.when(later < groups)
            def _():
                for step in chosen:
                    from_side(later, step)

        if len(waves) > hops + 1:
            pl.when(group == 0)(lambda: run(waves[-1:]))
        pl.when(ahead < groups)(lambda: from_far(ahead))
        query = (project(0) * HEAD ** (-0.5)).astype(jnp.bfloat16)
        keys = project(1).astype(jnp.bfloat16)
        contents = project(2).astype(jnp.bfloat16)
        bring(range(levels - 2))
        attend(group, 1, query, keys, contents)
        bring(range(levels - 2, levels))
        attend(group, 2, query, keys, contents)
        copies = returns(group)
        for copy in copies[: size_y - 1]:
            copy.start()
        attend(group, 0, query, keys, contents)
        for copy in copies[size_y - 1 :]:
            copy.start()
        pl.when(ahead < groups)(lambda: complete(ahead))
        return carry

    lax.fori_loop(0, groups, group_step, 0)
    keep_own(mixed.at[1], back_y, me_y, size_y)
    keep_own(mixed.at[2], back_z, me_z, size_z)

    def finish(group, carry):
        drain(group)
        for copy in returns(group):
            copy.wait()
        return carry

    lax.fori_loop(0, groups, finish, 0)
    summed = mixed[0].astype(jnp.float32) + back_y[...].astype(jnp.float32)
    summed = (summed + back_z[...].astype(jnp.float32)).astype(jnp.bfloat16)
    summed = summed.reshape(-1, features)
    for first in range(0, features, wide):
        cols = slice(first, first + wide)
        product = jnp.dot(summed, full[3, :, cols], preferred_element_type=jnp.float32)
        residual = tokens[:, :, cols].astype(jnp.float32)
        result[:, :, cols] = (residual + product.reshape(residual.shape)).astype(jnp.bfloat16)


VMEM = pl.BlockSpec(memory_space=pltpu.VMEM)
DMA = pltpu.SemaphoreType.DMA


def fast_shards(size_y, size_z, tokens, w_qkv, w_out, bias_x, bias_y, bias_z):
    samples, depth, rows_y, rows_z, features = tokens.shape
    rows = depth * rows_y * rows_z
    levels = size_y // 2
    groups = features // (4 * HEAD)
    lengths = [(table.shape[1] + 1) // 2 for table in (bias_x, bias_y, bias_z)]
    lookup = offset_lookup(line_places(rows, size_y, size_z, rows_z), lengths, rows)
    offsets = jnp.dot(
        jnp.concatenate([bias_x, bias_y, bias_z], axis=1), lookup, precision=lax.Precision.HIGHEST
    )
    weights = jnp.stack([w_qkv[:, n * features : (n + 1) * features] for n in range(3)] + [w_out])
    block = (samples, rows, features)
    result = pl.pallas_call(
        functools.partial(fused_kernel, size_y, size_z, rows_z),
        out_shape=jax.ShapeDtypeStruct(block, jnp.bfloat16),
        in_specs=[VMEM, VMEM, VMEM],
        out_specs=VMEM,
        scratch_shapes=[
            pltpu.VMEM((3,) + block, jnp.bfloat16),
            pltpu.VMEM((4, features, features), jnp.bfloat16),
            pltpu.VMEM((3, HEADS, rows, rows), jnp.float32),
            pltpu.VMEM((3,) + block, jnp.bfloat16),
            pltpu.VMEM(block, jnp.bfloat16),
            pltpu.VMEM(block, jnp.bfloat16),
            DMA((size_y - 1,)), DMA((size_y - 1,)), DMA((size_z - 1,)), DMA((size_z - 1,)),
            DMA((groups, levels)), DMA((groups, levels)), DMA((groups, levels)), DMA((groups, levels)),
            DMA((groups, levels)), DMA((groups, levels)),
            DMA((groups, size_y)), DMA((groups, size_y)),
            DMA((groups, size_y)), DMA((groups, size_y)),
            DMA((groups, size_y)), DMA((groups, size_y)),
            DMA((groups, size_y - 1)), DMA((groups, size_y - 1)),
            DMA((groups, size_z - 1)), DMA((groups, size_z - 1)),
        ],
        compiler_params=pltpu.CompilerParams(collective_id=0, has_side_effects=True),
    )(tokens.reshape(block), weights, offsets.reshape(groups, 4, 6 * rows))
    return result.reshape(tokens.shape)


def body_for(size_y, size_z):
    def body(tokens, *parameters):
        _, depth, rows_y, rows_z, features = tokens.shape
        rows = depth * rows_y * rows_z
        whole_parts = size_y % 2 == 0 and size_z % 4 == 0 and rows == 2 * HEAD
        if whole_parts and rows_y == 1 and rows % (16 * size_y) == 0 and rows % (16 * size_z) == 0:
            return fast_shards(size_y, size_z, tokens, *parameters)
        return shards(tokens, *parameters)

    return body


def solution(mesh):
    placed = (P(None, None, "gy", "gz", None), P("gy", None), P("gy", None), P(), P(), P())
    return jax.shard_map(
        body_for(mesh.shape["gy"], mesh.shape["gz"]),
        mesh=mesh,
        in_specs=placed,
        out_specs=P(None, None, "gy", "gz", None),
        check_vma=False,
    )
```
